16 devices in a mesh: rep: 4 (over y, z, core), dp: 4 (over x).
Axes of the slice: x: 4, y: 2, z: 1, core: 2. Of those that a mesh axis runs over, the one named last changes fastest.
The devices are a block of a 4x4x8 slice.
Arguments:
- g_w_gate: bfloat16 [16, 2, 512, 8192], P(('rep', 'dp')), parts along dimension 0
- g_w_up: bfloat16 [16, 2, 512, 8192], P(('rep', 'dp')), parts along dimension 0
- g_w_down: bfloat16 [16, 2, 8192, 512], P(('rep', 'dp')), parts along dimension 0
- w_gate: bfloat16 [2, 512, 8192], replicated
- w_up: bfloat16 [2, 512, 8192], replicated
- w_down: bfloat16 [2, 8192, 512], replicated
- m_w_gate: float32 [2, 512, 8192], P(None, 'dp')
- m_w_up: float32 [2, 512, 8192], P(None, 'dp')
- m_w_down: float32 [2, 8192, 512], P(None, 'dp')
- v_w_gate: float32 [2, 512, 8192], P(None, 'dp')
- v_w_up: float32 [2, 512, 8192], P(None, 'dp')
- v_w_down: float32 [2, 8192, 512], P(None, 'dp')
Outputs:
- output 1: bfloat16 [8, 512, 8192], P('rep'), parts along dimension 0
- output 2: bfloat16 [8, 512, 8192], P('rep'), parts along dimension 0
- output 3: bfloat16 [8, 8192, 512], P('rep'), parts along dimension 0
- output 4: float32 [8, 512, 8192], P('rep', 'dp'), parts along dimension 0
- output 5: float32 [8, 512, 8192], P('rep', 'dp'), parts along dimension 0
- output 6: float32 [8, 8192, 512], P('rep', 'dp'), parts along dimension 0
- output 7: float32 [8, 512, 8192], P('rep', 'dp'), parts along dimension 0
- output 8: float32 [8, 512, 8192], P('rep', 'dp'), parts along dimension 0
- output 9: float32 [8, 8192, 512], P('rep', 'dp'), parts along dimension 0
There are 4 independent parts. The reference program is written for one: setup_inputs(seed, part) draws one part's arguments, and reference() takes and returns one part's arrays. A program takes and returns all parts, laid end to end along the dimension named above; an argument that names none is the same for every part.
All inputs are finite; a program needn't handle non-finite values.
Results may differ from the reference program's by a relative error of at most 0.022.
Values are sent between devices in bfloat16 or wider.
A program may use at most 768 MiB of HBM per device.

```python
import jax
import jax.numpy as jnp
from jax import lax

DEVICES = 4
D = 512
FF = 8192
LAYERS = 2
NAMES = ("w_gate", "w_up", "w_down")
SHAPES = {"w_gate": (LAYERS, D, FF), "w_up": (LAYERS, D, FF), "w_down": (LAYERS, FF, D)}


def setup_inputs(seed: int = 0, part: int = 0) -> dict:
    kz, *keys = jax.random.split(jax.random.key(seed), 1 + 5 * len(NAMES))
    loud = 2.0 ** jax.random.uniform(kz, (), jnp.float32, -1.0, 1.0)
    drawn = {}
    for name, key, both in zip(NAMES, keys[:3], keys[3:6], strict=True):
        own = jax.random.normal(jax.random.fold_in(key, part), (DEVICES, *SHAPES[name]), jnp.float32)
        shared = jax.random.normal(jax.random.fold_in(both, part), SHAPES[name], jnp.float32)
        drawn["g_" + name] = (loud * (0.7 * shared / DEVICES + 0.7 * own * DEVICES**-0.5)).astype(jnp.bfloat16)
    for name, key in zip(NAMES, keys[6:9], strict=True):
        drawn[name] = (jax.random.normal(key, SHAPES[name], jnp.float32) * SHAPES[name][1] ** -0.5).astype(jnp.bfloat16)
    for name, key in zip(NAMES, keys[9:12], strict=True):
        drawn["m_" + name] = loud * 0.5 * jax.random.normal(key, SHAPES[name], jnp.float32)
    for name, key in zip(NAMES, keys[12:15], strict=True):
        drawn["v_" + name] = loud * loud * jax.random.uniform(key, SHAPES[name], jnp.float32, 0.5, 1.5)
    return drawn


def adamw(w, m, v, g):
    m = 0.9 * m + 0.1 * g
    v = 0.95 * v + 0.05 * g * g
    step = m * lax.rsqrt(v + 1e-8) + 0.1 * w
    return (w - 0.02 * step).astype(jnp.bfloat16), m, v


def reference(g_w_gate, g_w_up, g_w_down, w_gate, w_up, w_down, m_w_gate, m_w_up, m_w_down, v_w_gate, v_w_up, v_w_down):
    def total(terms):
        return lax.scan(lambda so_far, term: (so_far + term.astype(jnp.float32), None), jnp.zeros(terms.shape[1:], jnp.float32), terms)[0]

    gradients = [total(terms).astype(jnp.bfloat16).astype(jnp.float32) for terms in (g_w_gate, g_w_up, g_w_down)]
    new = [
        adamw(w.astype(jnp.float32), m, v, g)
        for w, m, v, g in zip((w_gate, w_up, w_down), (m_w_gate, m_w_up, m_w_down), (v_w_gate, v_w_up, v_w_down), gradients, strict=True)
    ]
    return tuple(one[which] for which in range(3) for one in new)
```

```python
import jax
import jax.numpy as jnp
from jax import lax
from jax.experimental import pallas as pl
from jax.experimental.pallas import tpu as pltpu
from jax.sharding import PartitionSpec as P


def adamw(w, m, v, g):
    m = 0.9 * m + 0.1 * g
    v = 0.95 * v + 0.05 * g * g
    step = m * lax.rsqrt(v + 1e-8) + 0.1 * w
    return (w - 0.02 * step).astype(jnp.bfloat16), m, v


def update(me, arrived, term, w, m, v):
    layers, rows, columns = m.shape
    half = rows // 2
    parts = max(1, half * columns * 4 // (1 << 20))
    tile = half // parts

    def kernel(me_ref, up_ref, down_ref, t_ref, w_ref, m_ref, v_ref, out_ref, m_out, v_out, up_out, down_out):
        for side, (in_ref, o_ref) in enumerate(((up_ref, up_out), (down_ref, down_out))):

            @pl.when(pl.program_id(1) == side)
            def _():
                g = (in_ref[0].astype(jnp.float32) + t_ref[0, 0].astype(jnp.float32)).astype(jnp.bfloat16)
                new, m_new, v_new = adamw(w_ref[0].astype(jnp.float32), m_ref[0], v_ref[0], g.astype(jnp.float32))
                out_ref[0], o_ref[0], m_out[0], v_out[0] = new, new, m_new, v_new

    def row(s, p):
        return s * parts + p

    up = pl.BlockSpec((1, tile, columns), lambda l, s, p, me: (l, jnp.where(s == 0, p, parts - 1), 0))
    down = pl.BlockSpec((1, tile, columns), lambda l, s, p, me: (l, jnp.where(s == 0, 0, p), 0))
    whole = pl.BlockSpec((1, tile, columns), lambda l, s, p, me: (l, me[0] * 2 * parts + row(s, p), 0))
    local = pl.BlockSpec((1, tile, columns), lambda l, s, p, me: (l, row(s, p), 0))
    t_spec = pl.BlockSpec((1, 1, tile, columns), lambda l, s, p, me: (0, l, me[0] * 2 * parts + row(s, p), 0))
    piece = jax.ShapeDtypeStruct((layers, half, columns), jnp.bfloat16)
    moment = jax.ShapeDtypeStruct(m.shape, jnp.float32)
    size = layers * rows * columns
    return pl.pallas_call(
        kernel,
        out_shape=(jax.ShapeDtypeStruct(w.shape, jnp.bfloat16), moment, moment, piece, piece),
        grid_spec=pltpu.PrefetchScalarGridSpec(
            num_scalar_prefetch=1,
            grid=(layers, 2, parts),
            in_specs=[up, down, t_spec, whole, local, local],
            out_specs=(whole, local, local, up, down),
        ),
        cost_estimate=pl.CostEstimate(flops=20 * size, bytes_accessed=26 * size, transcendentals=size),
        name="update",
    )(me, *arrived, term, w, m, v)


def place(blocks, whole, pieces):
    layers, half, columns = pieces[0].shape

    def kernel(at_ref, up_ref, down_ref, whole_ref, out_ref):
        for side, in_ref in enumerate((up_ref, down_ref)):

            @pl.when(pl.program_id(1) == side)
            def _():
                out_ref[...] = in_ref[...]

    block = (1, half, columns)
    size = 2 * layers * half * columns
    return pl.pallas_call(
        kernel,
        out_shape=jax.ShapeDtypeStruct(whole.shape, whole.dtype),
        grid_spec=pltpu.PrefetchScalarGridSpec(
            num_scalar_prefetch=1,
            grid=(layers, 2),
            in_specs=[
                pl.BlockSpec(block, lambda l, s, at: (l, 0, 0)),
                pl.BlockSpec(block, lambda l, s, at: (l, 0, 0)),
                pl.BlockSpec(memory_space=pl.ANY),
            ],
            out_specs=pl.BlockSpec(block, lambda l, s, at: (l, at[s] * 2 + s, 0)),
        ),
        input_output_aliases={3: 0},
        cost_estimate=pl.CostEstimate(flops=size, bytes_accessed=4 * size, transcendentals=0),
        name="place",
    )(blocks, *pieces, whole)


def solution(mesh):
    n = mesh.shape["dp"]
    ways = tuple(tuple((i, (i + to) % n) for i in range(n)) for to in (1, -1))

    def step(*arrays):
        terms, weights, m, v = (arrays[i : i + 3] for i in (0, 3, 6, 9))
        me = lax.axis_index("dp")
        sides = ((0, 1), (1, -1))

        def block(hops, to):
            return lax.rem(me - to * hops + 2 * n, n)

        def own(t, like, hops):
            rows = like.shape[1]
            half = rows // 2
            return [
                lax.dynamic_slice(t, (0, 0, block(-hops, to) * rows + side * half, 0), (1, t.shape[1], half, t.shape[3]))[0]
                for side, to in sides
            ]

        def send(pieces):
            return [lax.ppermute(p, "dp", way) for p, way in zip(pieces, ways, strict=True)]

        def add(a, b):
            return (a.astype(jnp.float32) + b.astype(jnp.float32)).astype(jnp.bfloat16)

        which = range(3)
        moving = [None] * 3
        new_w, new_m, new_v = [None] * 3, [None] * 3, [None] * 3
        for k in which:
            moving[k] = send(own(terms[k], m[k], n - 1))
        for hop in range(1, n - 1):
            for k in which:
                moving[k] = send([add(a, b) for a, b in zip(moving[k], own(terms[k], m[k], n - 1 - hop), strict=True)])
        at = me[None].astype(jnp.int32)
        for k in which:
            new_w[k], new_m[k], new_v[k], *pieces = update(at, moving[k], terms[k], weights[k], m[k], v[k])
            moving[k] = send(pieces)
        for hop in range(1, n):
            at = jnp.stack([block(hop, to) for _, to in sides]).astype(jnp.int32)
            for k in which:
                here = moving[k]
                if hop < n - 1:
                    moving[k] = send(here)
                new_w[k] = place(at, new_w[k], here)
        return (*new_w, *new_m, *new_v)

    all_of, cut = P(None, None, None), P(None, "dp", None)
    return jax.shard_map(
        step,
        mesh=mesh,
        in_specs=(P(("rep", "dp"), None, None, None),) * 3 + (all_of,) * 3 + (cut,) * 6,
        out_specs=(P("rep", None, None),) * 3 + (P("rep", "dp", None),) * 6,
        check_vma=False,
    )
```

```python
import jax
import jax.numpy as jnp
from jax import lax
from jax.experimental import pallas as pl
from jax.experimental.pallas import tpu as pltpu
from jax.sharding import PartitionSpec as P


def adamw(w, m, v, g):
    m = 0.9 * m + 0.1 * g
    v = 0.95 * v + 0.05 * g * g
    step = m * lax.rsqrt(v + 1e-8) + 0.1 * w
    return (w - 0.02 * step).astype(jnp.bfloat16), m, v


def update(me, arrived, term, w, m, v):
    layers, rows, columns = m.shape
    half = rows // 2
    parts = max(1, half * columns * 4 // (1 << 20))
    tile = half // parts

    def kernel(me_ref, up_ref, down_ref, t_ref, w_ref, m_ref, v_ref, out_ref, m_out, v_out, up_out, down_out):
        for side, (in_ref, o_ref) in enumerate(((up_ref, up_out), (down_ref, down_out))):

            @pl.when(pl.program_id(1) == side)
            def _():
                g = (in_ref[0].astype(jnp.float32) + t_ref[0, 0].astype(jnp.float32)).astype(jnp.bfloat16)
                new, m_new, v_new = adamw(w_ref[0].astype(jnp.float32), m_ref[0], v_ref[0], g.astype(jnp.float32))
                out_ref[0], o_ref[0], m_out[0], v_out[0] = new, new, m_new, v_new

    def row(s, p):
        return s * parts + p

    up = pl.BlockSpec((1, tile, columns), lambda l, s, p, me: (l, jnp.where(s == 0, p, parts - 1), 0))
    down = pl.BlockSpec((1, tile, columns), lambda l, s, p, me: (l, jnp.where(s == 0, 0, p), 0))
    whole = pl.BlockSpec((1, tile, columns), lambda l, s, p, me: (l, me[0] * 2 * parts + row(s, p), 0))
    local = pl.BlockSpec((1, tile, columns), lambda l, s, p, me: (l, row(s, p), 0))
    t_spec = pl.BlockSpec((1, 1, tile, columns), lambda l, s, p, me: (0, l, me[0] * 2 * parts + row(s, p), 0))
    piece = jax.ShapeDtypeStruct((layers, half, columns), jnp.bfloat16)
    moment = jax.ShapeDtypeStruct(m.shape, jnp.float32)
    size = layers * rows * columns
    return pl.pallas_call(
        kernel,
        out_shape=(jax.ShapeDtypeStruct(w.shape, jnp.bfloat16), moment, moment, piece, piece),
        grid_spec=pltpu.PrefetchScalarGridSpec(
            num_scalar_prefetch=1,
            grid=(layers, 2, parts),
            in_specs=[up, down, t_spec, whole, local, local],
            out_specs=(whole, local, local, up, down),
        ),
        cost_estimate=pl.CostEstimate(flops=20 * size, bytes_accessed=26 * size, transcendentals=size),
        name="update",
    )(me, *arrived, term, w, m, v)


def place(axis, hops, whole, pieces, layer, row, half, last):
    layers, rows, columns = pieces[0].shape
    count = whole.shape[1] // (2 * half)

    def kernel(up_ref, down_ref, whole_ref, out_ref, held, in_sems, out_sems):
        del whole_ref
        me = lax.axis_index(axis)
        reads, writes = [], []
        for side, ref in enumerate((up_ref, down_ref)):
            block = lax.rem(me + (count - hops, hops)[side], count)
            start = pl.multiple_of((block * 2 + side) * half, half) + row
            for i in range(layers):
                source = ref.at[i] if last else held.at[side, i]
                if not last:
                    reads.append(pltpu.make_async_copy(ref.at[i], source, in_sems.at[side, i]))
                writes.append(pltpu.make_async_copy(source, out_ref.at[layer + i, pl.ds(start, rows)], out_sems.at[side, i]))
        for read in reads:
            read.start()
        for i, write in enumerate(writes):
            if not last:
                reads[i].wait()
            write.start()
        for write in writes:
            write.wait()

    size = 2 * layers * rows * columns
    return pl.pallas_call(
        kernel,
        out_shape=jax.ShapeDtypeStruct(whole.shape, whole.dtype),
        in_specs=[pl.BlockSpec(memory_space=pltpu.VMEM if last else pl.ANY)] * 2 + [pl.BlockSpec(memory_space=pl.ANY)],
        out_specs=pl.BlockSpec(memory_space=pl.ANY),
        scratch_shapes=[
            pltpu.VMEM((8, 128) if last else (2, layers, rows, columns), whole.dtype),
            pltpu.SemaphoreType.DMA((2, layers)),
            pltpu.SemaphoreType.DMA((2, layers)),
        ],
        input_output_aliases={2: 0},
        compiler_params=pltpu.CompilerParams(vmem_limit_bytes=1 << 20 if last else None),
        cost_estimate=pl.CostEstimate(flops=size, bytes_accessed=4 * size, transcendentals=0),
        name="place",
    )(*pieces, whole)


def solution(mesh):
    n = mesh.shape["dp"]
    ways = tuple(tuple((i, (i + to) % n) for i in range(n)) for to in (1, -1))

    def body(*arrays):
        terms, weights, m, v = (arrays[i : i + 3] for i in (0, 3, 6, 9))
        me = lax.axis_index("dp")
        sides = ((0, 1), (1, -1))

        def block(hops, to):
            return lax.rem(me - to * hops + 2 * n, n)

        def own(t, like, hops, part):
            half, (layer, layers, row, rows) = like.shape[1] // 2, part
            starts = [block(-hops, to) * 2 * half + side * half + row for side, to in sides]
            return [lax.dynamic_slice(t, (0, layer, start, 0), (1, layers, rows, t.shape[3]))[0] for start in starts]

        def send(pieces):
            moved = []
            for p, way in zip(pieces, ways, strict=True):
                moved.append(lax.ppermute(p, "dp", way))
            return moved

        def add(a, b):
            return (a.astype(jnp.float32) + b.astype(jnp.float32)).astype(jnp.bfloat16)

        def all_of_it(like):
            return [(0, like.shape[0], 0, like.shape[1] // 2)]

        def small_first(like):
            layers, half = like.shape[0], like.shape[1] // 2
            return [(0, 1, 0, half // 4), (0, 1, half // 4, half - half // 4)] + [(1, layers - 1, 0, half)] * (layers > 1)

        def small_last(like):
            layers, half = like.shape[0], like.shape[1] // 2
            quarter = half // 4
            ends = [(layers - 1, 1, 0, half - 2 * quarter)] + [(layers - 1, 1, half - i * quarter, quarter) for i in (2, 1)]
            return [(0, layers - 1, 0, half)] * (layers > 1) + ends

        def join(parts):
            first = jnp.concatenate(parts[:2], axis=1)
            return jnp.concatenate([first, *parts[2:]], axis=0) if len(parts) > 2 else first

        order = (2, 1, 0)
        moving = [None] * 3
        new_w, new_m, new_v = [None] * 3, [None] * 3, [None] * 3
        for k in order:
            if k == order[0]:
                sent = [send(own(terms[k], m[k], n - 1, part)) for part in small_first(m[k])]
                moving[k] = [join(parts) for parts in zip(*sent, strict=True)]
            else:
                moving[k] = send(own(terms[k], m[k], n - 1, all_of_it(m[k])[0]))
        for hop in range(1, n - 1):
            for k in order:
                moving[k] = send([add(a, b) for a, b in zip(moving[k], own(terms[k], m[k], n - 1 - hop, all_of_it(m[k])[0]), strict=True)])
        at = me[None].astype(jnp.int32)
        for k in order:
            new_w[k], new_m[k], new_v[k], *pieces = update(at, moving[k], terms[k], weights[k], m[k], v[k])
            moving[k] = [(part, send(pieces)) for part in all_of_it(m[k])]
        for hop in range(1, n):
            for k in order:
                here = moving[k]
                if hop < n - 1:
                    parts = small_last(m[k]) if (hop, k) == (n - 2, order[-1]) else all_of_it(m[k])
                    ((_, whole_piece),) = here
                    moving[k] = [
                        (part, send([p[part[0] : part[0] + part[1], part[2] : part[2] + part[3]] for p in whole_piece])) for part in parts
                    ]
                for i, (part, pieces) in enumerate(here):
                    last = (hop, k, i) == (n - 1, order[-1], len(here) - 1)
                    new_w[k] = place("dp", hop, new_w[k], pieces, part[0], part[2], m[k].shape[1] // 2, last)
        return (*new_w, *new_m, *new_v)

    all_of, cut = P(None, None, None), P(None, "dp", None)
    return jax.shard_map(
        body,
        mesh=mesh,
        in_specs=(P(("rep", "dp"), None, None, None),) * 3 + (all_of,) * 3 + (cut,) * 6,
        out_specs=(P("rep", None, None),) * 3 + (P("rep", "dp", None),) * 6,
        check_vma=False,
    )
```

```python
import jax
import jax.numpy as jnp
from jax import lax
from jax.experimental import pallas as pl
from jax.experimental.pallas import tpu as pltpu
from jax.sharding import PartitionSpec as P


def adamw(w, m, v, g):
    m = 0.9 * m + 0.1 * g
    v = 0.95 * v + 0.05 * g * g
    step = m * lax.rsqrt(v + 1e-8) + 0.1 * w
    return (w - 0.02 * step).astype(jnp.bfloat16), m, v


def update(me, arrived, term, w, m, v):
    layers, rows, columns = m.shape
    half = rows // 2
    parts = max(1, half * columns * 4 // (1 << 20))
    tile = half // parts

    def kernel(me_ref, up_ref, down_ref, t_ref, w_ref, m_ref, v_ref, out_ref, m_out, v_out, up_out, down_out):
        for side, (in_ref, o_ref) in enumerate(((up_ref, up_out), (down_ref, down_out))):

            @pl.when(pl.program_id(1) == side)
            def _():
                g = (in_ref[0].astype(jnp.float32) + t_ref[0, 0].astype(jnp.float32)).astype(jnp.bfloat16)
                new, m_new, v_new = adamw(w_ref[0].astype(jnp.float32), m_ref[0], v_ref[0], g.astype(jnp.float32))
                out_ref[0], o_ref[0], m_out[0], v_out[0] = new, new, m_new, v_new

    def row(s, p):
        return s * parts + p

    up = pl.BlockSpec((1, tile, columns), lambda l, s, p, me: (l, jnp.where(s == 0, p, parts - 1), 0))
    down = pl.BlockSpec((1, tile, columns), lambda l, s, p, me: (l, jnp.where(s == 0, 0, p), 0))
    whole = pl.BlockSpec((1, tile, columns), lambda l, s, p, me: (l, me[0] * 2 * parts + row(s, p), 0))
    local = pl.BlockSpec((1, tile, columns), lambda l, s, p, me: (l, row(s, p), 0))
    t_spec = pl.BlockSpec((1, 1, tile, columns), lambda l, s, p, me: (0, l, me[0] * 2 * parts + row(s, p), 0))
    piece = jax.ShapeDtypeStruct((layers, half, columns), jnp.bfloat16)
    moment = jax.ShapeDtypeStruct(m.shape, jnp.float32)
    size = layers * rows * columns
    return pl.pallas_call(
        kernel,
        out_shape=(jax.ShapeDtypeStruct(w.shape, jnp.bfloat16), moment, moment, piece, piece),
        grid_spec=pltpu.PrefetchScalarGridSpec(
            num_scalar_prefetch=1,
            grid=(layers, 2, parts),
            in_specs=[up, down, t_spec, whole, local, local],
            out_specs=(whole, local, local, up, down),
        ),
        cost_estimate=pl.CostEstimate(flops=20 * size, bytes_accessed=26 * size, transcendentals=size),
        name="update",
    )(me, *arrived, term, w, m, v)


def place(axis, hops, whole, pieces, layer, row, half, last):
    layers, rows, columns = pieces[0].shape
    count = whole.shape[1] // (2 * half)

    def kernel(up_ref, down_ref, whole_ref, out_ref, held, in_sems, out_sems):
        del whole_ref
        me = lax.axis_index(axis)
        reads, writes = [], []
        for side, ref in enumerate((up_ref, down_ref)):
            block = lax.rem(me + (count - hops, hops)[side], count)
            start = pl.multiple_of((block * 2 + side) * half, half) + row
            for i in range(layers):
                source = ref.at[i] if last else held.at[side, i]
                if not last:
                    reads.append(pltpu.make_async_copy(ref.at[i], source, in_sems.at[side, i]))
                writes.append(pltpu.make_async_copy(source, out_ref.at[layer + i, pl.ds(start, rows)], out_sems.at[side, i]))
        for read in reads:
            read.start()
        for i, write in enumerate(writes):
            if not last:
                reads[i].wait()
            write.start()
        for write in writes:
            write.wait()

    size = 2 * layers * rows * columns
    return pl.pallas_call(
        kernel,
        out_shape=jax.ShapeDtypeStruct(whole.shape, whole.dtype),
        in_specs=[pl.BlockSpec(memory_space=pltpu.VMEM if last else pl.ANY)] * 2 + [pl.BlockSpec(memory_space=pl.ANY)],
        out_specs=pl.BlockSpec(memory_space=pl.ANY),
        scratch_shapes=[
            pltpu.VMEM((8, 128) if last else (2, layers, rows, columns), whole.dtype),
            pltpu.SemaphoreType.DMA((2, layers)),
            pltpu.SemaphoreType.DMA((2, layers)),
        ],
        input_output_aliases={2: 0},
        compiler_params=pltpu.CompilerParams(vmem_limit_bytes=1 << 20 if last else None),
        cost_estimate=pl.CostEstimate(flops=size, bytes_accessed=4 * size, transcendentals=0),
        name="place",
    )(*pieces, whole)


def first_slice(axis, hops, term, half, rows):
    columns = term.shape[3]
    count = term.shape[2] // (2 * half)

    def kernel(term_ref, up_ref, down_ref, sems):
        me = lax.axis_index(axis)
        copies = []
        for side, ref in enumerate((up_ref, down_ref)):
            block = lax.rem(me + (hops, count - hops)[side], count)
            start = pl.multiple_of((block * 2 + side) * half, half)
            copies.append(pltpu.make_async_copy(term_ref.at[0, 0, pl.ds(start, rows)], ref.at[0], sems.at[side]))
        for copy in copies:
            copy.start()
        for copy in copies:
            copy.wait()

    piece = jax.ShapeDtypeStruct((1, rows, columns), term.dtype)
    return pl.pallas_call(
        kernel,
        out_shape=(piece, piece),
        in_specs=[pl.BlockSpec(memory_space=pl.ANY)],
        out_specs=(pl.BlockSpec(memory_space=pltpu.VMEM),) * 2,
        scratch_shapes=[pltpu.SemaphoreType.DMA((2,))],
        compiler_params=pltpu.CompilerParams(vmem_limit_bytes=52 << 20),
        cost_estimate=pl.CostEstimate(flops=rows * columns, bytes_accessed=8 * rows * columns, transcendentals=0),
        name="first_slice",
    )(term)


def solution(mesh):
    n = mesh.shape["dp"]
    ways = tuple(tuple((i, (i + to) % n) for i in range(n)) for to in (1, -1))

    def body(*arrays):
        terms, weights, m, v = (arrays[i : i + 3] for i in (0, 3, 6, 9))
        me = lax.axis_index("dp")
        sides = ((0, 1), (1, -1))

        def block(hops, to):
            return lax.rem(me - to * hops + 2 * n, n)

        def own(t, like, hops, part):
            half, (layer, layers, row, rows) = like.shape[1] // 2, part
            starts = [block(-hops, to) * 2 * half + side * half + row for side, to in sides]
            return [lax.dynamic_slice(t, (0, layer, start, 0), (1, layers, rows, t.shape[3]))[0] for start in starts]

        def send(pieces):
            moved = []
            for p, way in zip(pieces, ways, strict=True):
                moved.append(lax.ppermute(p, "dp", way))
            return moved

        def add(a, b):
            return (a.astype(jnp.float32) + b.astype(jnp.float32)).astype(jnp.bfloat16)

        def all_of_it(like):
            return [(0, like.shape[0], 0, like.shape[1] // 2)]

        def small_first(like):
            layers, half = like.shape[0], like.shape[1] // 2
            return [(0, 1, 0, half // 4), (0, 1, half // 4, half - half // 4)] + [(1, layers - 1, 0, half)] * (layers > 1)

        def small_last(like):
            layers, half = like.shape[0], like.shape[1] // 2
            quarter = half // 4
            ends = [(layers - 1, 1, 0, half - 2 * quarter)] + [(layers - 1, 1, half - i * quarter, quarter) for i in (2, 1)]
            return [(0, layers - 1, 0, half)] * (layers > 1) + ends

        def join(parts):
            first = jnp.concatenate(parts[:2], axis=1)
            return jnp.concatenate([first, *parts[2:]], axis=0) if len(parts) > 2 else first

        order = (2, 1, 0)
        moving = [None] * 3
        new_w, new_m, new_v = [None] * 3, [None] * 3, [None] * 3
        for k in order:
            if k == order[0]:
                half, parts = m[k].shape[1] // 2, small_first(m[k])
                sent = [send(first_slice("dp", n - 1, terms[k], half, parts[0][3]))]
                sent += [send(own(terms[k], m[k], n - 1, part)) for part in parts[1:]]
                moving[k] = [join(parts) for parts in zip(*sent, strict=True)]
            else:
                moving[k] = send(own(terms[k], m[k], n - 1, all_of_it(m[k])[0]))
        for hop in range(1, n - 1):
            for k in order:
                moving[k] = send([add(a, b) for a, b in zip(moving[k], own(terms[k], m[k], n - 1 - hop, all_of_it(m[k])[0]), strict=True)])
        at = me[None].astype(jnp.int32)
        for k in order:
            new_w[k], new_m[k], new_v[k], *pieces = update(at, moving[k], terms[k], weights[k], m[k], v[k])
            moving[k] = [(part, send(pieces)) for part in all_of_it(m[k])]
        for hop in range(1, n):
            for k in order:
                here = moving[k]
                if hop < n - 1:
                    parts = small_last(m[k]) if (hop, k) == (n - 2, order[-1]) else all_of_it(m[k])
                    ((_, whole_piece),) = here
                    moving[k] = [
                        (part, send([p[part[0] : part[0] + part[1], part[2] : part[2] + part[3]] for p in whole_piece])) for part in parts
                    ]
                for i, (part, pieces) in enumerate(here):
                    last = (hop, k, i) == (n - 1, order[-1], len(here) - 1)
                    new_w[k] = place("dp", hop, new_w[k], pieces, part[0], part[2], m[k].shape[1] // 2, last)
        return (*new_w, *new_m, *new_v)

    all_of, cut = P(None, None, None), P(None, "dp", None)
    return jax.shard_map(
        body,
        mesh=mesh,
        in_specs=(P(("rep", "dp"), None, None, None),) * 3 + (all_of,) * 3 + (cut,) * 6,
        out_specs=(P("rep", None, None),) * 3 + (P("rep", "dp", None),) * 6,
        check_vma=False,
    )
```

```python
import jax
import jax.numpy as jnp
from jax import lax
from jax.experimental import pallas as pl
from jax.experimental.pallas import tpu as pltpu
from jax.sharding import PartitionSpec as P


def adamw(w, m, v, g):
    m = 0.9 * m + 0.1 * g
    v = 0.95 * v + 0.05 * g * g
    step = m * lax.rsqrt(v + 1e-8) + 0.1 * w
    return (w - 0.02 * step).astype(jnp.bfloat16), m, v


def update(me, arrived, term, w, m, v):
    layers, rows, columns = m.shape
    half = rows // 2
    parts = max(1, half * columns * 4 // (1 << 20))
    tile = half // parts

    def kernel(me_ref, up_ref, down_ref, t_ref, w_ref, m_ref, v_ref, out_ref, m_out, v_out, up_out, down_out):
        for side, (in_ref, o_ref) in enumerate(((up_ref, up_out), (down_ref, down_out))):

            @pl.when(pl.program_id(1) == side)
            def _():
                g = (in_ref[0].astype(jnp.float32) + t_ref[0, 0].astype(jnp.float32)).astype(jnp.bfloat16)
                new, m_new, v_new = adamw(w_ref[0].astype(jnp.float32), m_ref[0], v_ref[0], g.astype(jnp.float32))
                out_ref[0], o_ref[0], m_out[0], v_out[0] = new, new, m_new, v_new

    def row(s, p):
        return s * parts + p

    up = pl.BlockSpec((1, tile, columns), lambda l, s, p, me: (l, jnp.where(s == 0, p, parts - 1), 0))
    down = pl.BlockSpec((1, tile, columns), lambda l, s, p, me: (l, jnp.where(s == 0, 0, p), 0))
    whole = pl.BlockSpec((1, tile, columns), lambda l, s, p, me: (l, me[0] * 2 * parts + row(s, p), 0))
    local = pl.BlockSpec((1, tile, columns), lambda l, s, p, me: (l, row(s, p), 0))
    t_spec = pl.BlockSpec((1, 1, tile, columns), lambda l, s, p, me: (0, l, me[0] * 2 * parts + row(s, p), 0))
    piece = jax.ShapeDtypeStruct((layers, half, columns), jnp.bfloat16)
    moment = jax.ShapeDtypeStruct(m.shape, jnp.float32)
    size = layers * rows * columns
    return pl.pallas_call(
        kernel,
        out_shape=(jax.ShapeDtypeStruct(w.shape, jnp.bfloat16), moment, moment, piece, piece),
        grid_spec=pltpu.PrefetchScalarGridSpec(
            num_scalar_prefetch=1,
            grid=(layers, 2, parts),
            in_specs=[up, down, t_spec, whole, local, local],
            out_specs=(whole, local, local, up, down),
        ),
        cost_estimate=pl.CostEstimate(flops=20 * size, bytes_accessed=26 * size, transcendentals=size),
        name="update",
    )(me, *arrived, term, w, m, v)


def place(axis, hops, whole, pieces, layer, row, half, last):
    layers, rows, columns = pieces[0].shape
    count = whole.shape[1] // (2 * half)

    def kernel(up_ref, down_ref, whole_ref, out_ref, held, in_sems, out_sems):
        del whole_ref
        me = lax.axis_index(axis)
        reads, writes = [], []
        for side, ref in enumerate((up_ref, down_ref)):
            block = lax.rem(me + (count - hops, hops)[side], count)
            start = pl.multiple_of((block * 2 + side) * half, half) + row
            for i in range(layers):
                source = ref.at[i] if last else held.at[side, i]
                if not last:
                    reads.append(pltpu.make_async_copy(ref.at[i], source, in_sems.at[side, i]))
                writes.append(pltpu.make_async_copy(source, out_ref.at[layer + i, pl.ds(start, rows)], out_sems.at[side, i]))
        for read in reads:
            read.start()
        for i, write in enumerate(writes):
            if not last:
                reads[i].wait()
            write.start()
        for write in writes:
            write.wait()

    size = 2 * layers * rows * columns
    return pl.pallas_call(
        kernel,
        out_shape=jax.ShapeDtypeStruct(whole.shape, whole.dtype),
        in_specs=[pl.BlockSpec(memory_space=pltpu.VMEM if last else pl.ANY)] * 2 + [pl.BlockSpec(memory_space=pl.ANY)],
        out_specs=pl.BlockSpec(memory_space=pl.ANY),
        scratch_shapes=[
            pltpu.VMEM((8, 128) if last else (2, layers, rows, columns), whole.dtype),
            pltpu.SemaphoreType.DMA((2, layers)),
            pltpu.SemaphoreType.DMA((2, layers)),
        ],
        input_output_aliases={2: 0},
        compiler_params=pltpu.CompilerParams(vmem_limit_bytes=1 << 20 if last else None),
        cost_estimate=pl.CostEstimate(flops=size, bytes_accessed=4 * size, transcendentals=0),
        name="place",
    )(*pieces, whole)


def first_slice(axis, hops, term, half, rows):
    columns = term.shape[3]
    count = term.shape[2] // (2 * half)

    def kernel(term_ref, up_ref, down_ref, sems):
        me = lax.axis_index(axis)
        copies = []
        for side, ref in enumerate((up_ref, down_ref)):
            block = lax.rem(me + (hops, count - hops)[side], count)
            start = pl.multiple_of((block * 2 + side) * half, half)
            copies.append(pltpu.make_async_copy(term_ref.at[0, 0, pl.ds(start, rows)], ref.at[0], sems.at[side]))
        for copy in copies:
            copy.start()
        for copy in copies:
            copy.wait()

    piece = jax.ShapeDtypeStruct((1, rows, columns), term.dtype)
    return pl.pallas_call(
        kernel,
        out_shape=(piece, piece),
        in_specs=[pl.BlockSpec(memory_space=pl.ANY)],
        out_specs=(pl.BlockSpec(memory_space=pltpu.VMEM),) * 2,
        scratch_shapes=[pltpu.SemaphoreType.DMA((2,))],
        compiler_params=pltpu.CompilerParams(vmem_limit_bytes=52 << 20),
        cost_estimate=pl.CostEstimate(flops=rows * columns, bytes_accessed=8 * rows * columns, transcendentals=0),
        name="first_slice",
    )(term)


def solution(mesh):
    n = mesh.shape["dp"]
    ways = tuple(tuple((i, (i + to) % n) for i in range(n)) for to in (1, -1))

    def body(*arrays):
        terms, weights, m, v = (arrays[i : i + 3] for i in (0, 3, 6, 9))
        me = lax.axis_index("dp")
        sides = ((0, 1), (1, -1))

        def block(hops, to):
            return lax.rem(me - to * hops + 2 * n, n)

        def own(t, like, hops, part):
            half, (layer, layers, row, rows) = like.shape[1] // 2, part
            starts = [block(-hops, to) * 2 * half + side * half + row for side, to in sides]
            return [lax.dynamic_slice(t, (0, layer, start, 0), (1, layers, rows, t.shape[3]))[0] for start in starts]

        def send(pieces):
            moved = []
            for p, way in zip(pieces, ways, strict=True):
                moved.append(lax.ppermute(p, "dp", way))
            return moved

        def add(a, b):
            return (a.astype(jnp.float32) + b.astype(jnp.float32)).astype(jnp.bfloat16)

        def all_of_it(like):
            return [(0, like.shape[0], 0, like.shape[1] // 2)]

        def small_first(like):
            layers, half = like.shape[0], like.shape[1] // 2
            return [(0, 1, 0, half // 4), (0, 1, half // 4, half - half // 4)] + [(1, layers - 1, 0, half)] * (layers > 1)

        def small_last(like):
            layers, half = like.shape[0], like.shape[1] // 2
            quarter = half // 4
            small = quarter // 2
            ends = [(layers - 1, 1, 0, half - 3 * small), (layers - 1, 1, half - 3 * small, 2 * small), (layers - 1, 1, half - small, small)]
            return [(0, layers - 1, 0, half)] * (layers > 1) + ends

        def join(parts):
            first = jnp.concatenate(parts[:2], axis=1)
            return jnp.concatenate([first, *parts[2:]], axis=0) if len(parts) > 2 else first

        order = (0, 1, 2)
        moving = [None] * 3
        new_w, new_m, new_v = [None] * 3, [None] * 3, [None] * 3
        for k in order:
            if k == order[0]:
                half, parts = m[k].shape[1] // 2, small_first(m[k])
                sent = [send(first_slice("dp", n - 1, terms[k], half, parts[0][3]))]
                sent += [send(own(terms[k], m[k], n - 1, part)) for part in parts[1:]]
                moving[k] = [join(parts) for parts in zip(*sent, strict=True)]
            else:
                moving[k] = send(own(terms[k], m[k], n - 1, all_of_it(m[k])[0]))
        for hop in range(1, n - 1):
            for k in order:
                moving[k] = send([add(a, b) for a, b in zip(moving[k], own(terms[k], m[k], n - 1 - hop, all_of_it(m[k])[0]), strict=True)])
        at = me[None].astype(jnp.int32)
        for k in order:
            new_w[k], new_m[k], new_v[k], *pieces = update(at, moving[k], terms[k], weights[k], m[k], v[k])
            moving[k] = [(part, send(pieces)) for part in all_of_it(m[k])]
        for hop in range(1, n):
            for k in order:
                here = moving[k]
                if hop < n - 1:
                    parts = small_last(m[k]) if (hop, k) == (n - 2, order[-1]) else all_of_it(m[k])
                    ((_, whole_piece),) = here
                    moving[k] = [
                        (part, send([p[part[0] : part[0] + part[1], part[2] : part[2] + part[3]] for p in whole_piece])) for part in parts
                    ]
                for i, (part, pieces) in enumerate(here):
                    last = (hop, k) == (n - 1, order[-1]) and i >= len(here) - 2
                    new_w[k] = place("dp", hop, new_w[k], pieces, part[0], part[2], m[k].shape[1] // 2, last)
        return (*new_w, *new_m, *new_v)

    all_of, cut = P(None, None, None), P(None, "dp", None)
    return jax.shard_map(
        body,
        mesh=mesh,
        in_specs=(P(("rep", "dp"), None, None, None),) * 3 + (all_of,) * 3 + (cut,) * 6,
        out_specs=(P("rep", None, None),) * 3 + (P("rep", "dp", None),) * 6,
        check_vma=False,
    )
```

```python
import jax
import jax.numpy as jnp
from jax import lax
from jax.experimental import pallas as pl
from jax.experimental.pallas import tpu as pltpu
from jax.sharding import PartitionSpec as P


def adamw(w, m, v, g):
    m = 0.9 * m + 0.1 * g
    v = 0.95 * v + 0.05 * g * g
    step = m * lax.rsqrt(v + 1e-8) + 0.1 * w
    return (w - 0.02 * step).astype(jnp.bfloat16), m, v


def update(me, arrived, term, w, m, v):
    layers, rows, columns = m.shape
    half = rows // 2
    parts = max(1, half * columns * 4 // (1 << 20))
    tile = half // parts

    def kernel(me_ref, up_ref, down_ref, t_ref, w_ref, m_ref, v_ref, out_ref, m_out, v_out, up_out, down_out):
        for side, (in_ref, o_ref) in enumerate(((up_ref, up_out), (down_ref, down_out))):

            @pl.when(pl.program_id(1) == side)
            def _():
                g = (in_ref[0].astype(jnp.float32) + t_ref[0, 0].astype(jnp.float32)).astype(jnp.bfloat16)
                new, m_new, v_new = adamw(w_ref[0].astype(jnp.float32), m_ref[0], v_ref[0], g.astype(jnp.float32))
                out_ref[0], o_ref[0], m_out[0], v_out[0] = new, new, m_new, v_new

    def row(s, p):
        return s * parts + p

    up = pl.BlockSpec((1, tile, columns), lambda l, s, p, me: (l, jnp.where(s == 0, p, parts - 1), 0))
    down = pl.BlockSpec((1, tile, columns), lambda l, s, p, me: (l, jnp.where(s == 0, 0, p), 0))
    whole = pl.BlockSpec((1, tile, columns), lambda l, s, p, me: (l, me[0] * 2 * parts + row(s, p), 0))
    local = pl.BlockSpec((1, tile, columns), lambda l, s, p, me: (l, row(s, p), 0))
    t_spec = pl.BlockSpec((1, 1, tile, columns), lambda l, s, p, me: (0, l, me[0] * 2 * parts + row(s, p), 0))
    piece = jax.ShapeDtypeStruct((layers, half, columns), jnp.bfloat16)
    moment = jax.ShapeDtypeStruct(m.shape, jnp.float32)
    size = layers * rows * columns
    return pl.pallas_call(
        kernel,
        out_shape=(jax.ShapeDtypeStruct(w.shape, jnp.bfloat16), moment, moment, piece, piece),
        grid_spec=pltpu.PrefetchScalarGridSpec(
            num_scalar_prefetch=1,
            grid=(layers, 2, parts),
            in_specs=[up, down, t_spec, whole, local, local],
            out_specs=(whole, local, local, up, down),
        ),
        cost_estimate=pl.CostEstimate(flops=20 * size, bytes_accessed=26 * size, transcendentals=size),
        name="update",
    )(me, *arrived, term, w, m, v)


def place(axis, hops, whole, pieces, layer, row, half, last):
    layers, rows, columns = pieces[0].shape
    count = whole.shape[1] // (2 * half)

    def kernel(up_ref, down_ref, whole_ref, out_ref, held, in_sems, out_sems):
        del whole_ref
        me = lax.axis_index(axis)
        reads, writes = [], []
        for side, ref in enumerate((up_ref, down_ref)):
            block = lax.rem(me + (count - hops, hops)[side], count)
            start = pl.multiple_of((block * 2 + side) * half, half) + row
            for i in range(layers):
                source = ref.at[i] if last else held.at[side, i]
                if not last:
                    reads.append(pltpu.make_async_copy(ref.at[i], source, in_sems.at[side, i]))
                writes.append(pltpu.make_async_copy(source, out_ref.at[layer + i, pl.ds(start, rows)], out_sems.at[side, i]))
        for read in reads:
            read.start()
        for i, write in enumerate(writes):
            if not last:
                reads[i].wait()
            write.start()
        for write in writes:
            write.wait()

    size = 2 * layers * rows * columns
    return pl.pallas_call(
        kernel,
        out_shape=jax.ShapeDtypeStruct(whole.shape, whole.dtype),
        in_specs=[pl.BlockSpec(memory_space=pltpu.VMEM if last else pl.ANY)] * 2 + [pl.BlockSpec(memory_space=pl.ANY)],
        out_specs=pl.BlockSpec(memory_space=pl.ANY),
        scratch_shapes=[
            pltpu.VMEM((8, 128) if last else (2, layers, rows, columns), whole.dtype),
            pltpu.SemaphoreType.DMA((2, layers)),
            pltpu.SemaphoreType.DMA((2, layers)),
        ],
        input_output_aliases={2: 0},
        compiler_params=pltpu.CompilerParams(vmem_limit_bytes=1 << 20 if last else None),
        cost_estimate=pl.CostEstimate(flops=size, bytes_accessed=4 * size, transcendentals=0),
        name="place",
    )(*pieces, whole)


def first_slice(axis, hops, term, half, row, rows):
    columns = term.shape[3]
    count = term.shape[2] // (2 * half)

    def kernel(term_ref, up_ref, down_ref, sems):
        me = lax.axis_index(axis)
        copies = []
        for side, ref in enumerate((up_ref, down_ref)):
            block = lax.rem(me + (hops, count - hops)[side], count)
            start = pl.multiple_of((block * 2 + side) * half, half) + row
            copies.append(pltpu.make_async_copy(term_ref.at[0, 0, pl.ds(start, rows)], ref.at[0], sems.at[side]))
        for copy in copies:
            copy.start()
        for copy in copies:
            copy.wait()

    piece = jax.ShapeDtypeStruct((1, rows, columns), term.dtype)
    return pl.pallas_call(
        kernel,
        out_shape=(piece, piece),
        in_specs=[pl.BlockSpec(memory_space=pl.ANY)],
        out_specs=(pl.BlockSpec(memory_space=pltpu.VMEM),) * 2,
        scratch_shapes=[pltpu.SemaphoreType.DMA((2,))],
        compiler_params=pltpu.CompilerParams(vmem_limit_bytes=52 << 20),
        cost_estimate=pl.CostEstimate(flops=rows * columns, bytes_accessed=8 * rows * columns, transcendentals=0),
        name="first_slice",
    )(term)


def solution(mesh):
    n = mesh.shape["dp"]
    ways = tuple(tuple((i, (i + to) % n) for i in range(n)) for to in (1, -1))

    def body(*arrays):
        terms, weights, m, v = (arrays[i : i + 3] for i in (0, 3, 6, 9))
        me = lax.axis_index("dp")
        sides = ((0, 1), (1, -1))

        def block(hops, to):
            return lax.rem(me - to * hops + 2 * n, n)

        def own(t, like, hops, part):
            half, (layer, layers, row, rows) = like.shape[1] // 2, part
            starts = [block(-hops, to) * 2 * half + side * half + row for side, to in sides]
            return [lax.dynamic_slice(t, (0, layer, start, 0), (1, layers, rows, t.shape[3]))[0] for start in starts]

        def send(pieces):
            moved = []
            for p, way in zip(pieces, ways, strict=True):
                moved.append(lax.ppermute(p, "dp", way))
            return moved

        def add(a, b):
            return (a.astype(jnp.float32) + b.astype(jnp.float32)).astype(jnp.bfloat16)

        def all_of_it(like):
            return [(0, like.shape[0], 0, like.shape[1] // 2)]

        def small_first(like):
            layers, half = like.shape[0], like.shape[1] // 2
            return [(0, 1, 0, half // 4), (0, 1, half // 4, half - half // 4)] + [(1, layers - 1, 0, half)] * (layers > 1)

        def small_last(like):
            layers, half = like.shape[0], like.shape[1] // 2
            quarter = half // 4
            small = quarter // 2
            ends = [(layers - 1, 1, 0, half - 3 * small), (layers - 1, 1, half - 3 * small, 2 * small), (layers - 1, 1, half - small, small)]
            return [(0, layers - 1, 0, half)] * (layers > 1) + ends

        def join(parts):
            first = jnp.concatenate(parts[:2], axis=1)
            return jnp.concatenate([first, *parts[2:]], axis=0) if len(parts) > 2 else first

        order = (0, 1, 2)
        moving = [None] * 3
        new_w, new_m, new_v = [None] * 3, [None] * 3, [None] * 3
        for k in order:
            if k == order[0]:
                half, parts = m[k].shape[1] // 2, small_first(m[k])
                sent = [send(first_slice("dp", n - 1, terms[k], half, row, rows)) for _, _, row, rows in parts[:2]]
                sent += [send(own(terms[k], m[k], n - 1, part)) for part in parts[2:]]
                moving[k] = [join(parts) for parts in zip(*sent, strict=True)]
            else:
                moving[k] = send(own(terms[k], m[k], n - 1, all_of_it(m[k])[0]))
        for hop in range(1, n - 1):
            for k in order:
                moving[k] = send([add(a, b) for a, b in zip(moving[k], own(terms[k], m[k], n - 1 - hop, all_of_it(m[k])[0]), strict=True)])
        at = me[None].astype(jnp.int32)
        for k in order:
            new_w[k], new_m[k], new_v[k], *pieces = update(at, moving[k], terms[k], weights[k], m[k], v[k])
            moving[k] = [(part, send(pieces)) for part in all_of_it(m[k])]
        for hop in range(1, n):
            for k in order:
                here = moving[k]
                if hop < n - 1:
                    parts = small_last(m[k]) if (hop, k) == (n - 2, order[-1]) else all_of_it(m[k])
                    ((_, whole_piece),) = here
                    moving[k] = [
                        (part, send([p[part[0] : part[0] + part[1], part[2] : part[2] + part[3]] for p in whole_piece])) for part in parts
                    ]
                for i, (part, pieces) in enumerate(here):
                    last = (hop, k) == (n - 1, order[-1]) and i >= len(here) - 2
                    new_w[k] = place("dp", hop, new_w[k], pieces, part[0], part[2], m[k].shape[1] // 2, last)
        return (*new_w, *new_m, *new_v)

    all_of, cut = P(None, None, None), P(None, "dp", None)
    return jax.shard_map(
        body,
        mesh=mesh,
        in_specs=(P(("rep", "dp"), None, None, None),) * 3 + (all_of,) * 3 + (cut,) * 6,
        out_specs=(P("rep", None, None),) * 3 + (P("rep", "dp", None),) * 6,
        check_vma=False,
    )
```

```python
import jax
import jax.numpy as jnp
from jax import lax
from jax.experimental import pallas as pl
from jax.experimental.pallas import tpu as pltpu
from jax.sharding import PartitionSpec as P


def adamw(w, m, v, g):
    m = 0.9 * m + 0.1 * g
    v = 0.95 * v + 0.05 * g * g
    step = m * lax.rsqrt(v + 1e-8) + 0.1 * w
    return (w - 0.02 * step).astype(jnp.bfloat16), m, v


def update(me, arrived, term, w, m, v):
    layers, rows, columns = m.shape
    half = rows // 2
    parts = max(1, half * columns * 4 // (1 << 20))
    tile = half // parts

    def kernel(me_ref, up_ref, down_ref, t_ref, w_ref, m_ref, v_ref, out_ref, m_out, v_out, up_out, down_out):
        for side, (in_ref, o_ref) in enumerate(((up_ref, up_out), (down_ref, down_out))):

            @pl.when(pl.program_id(1) == side)
            def _():
                g = (in_ref[0].astype(jnp.float32) + t_ref[0, 0].astype(jnp.float32)).astype(jnp.bfloat16)
                new, m_new, v_new = adamw(w_ref[0].astype(jnp.float32), m_ref[0], v_ref[0], g.astype(jnp.float32))
                out_ref[0], o_ref[0], m_out[0], v_out[0] = new, new, m_new, v_new

    def row(s, p):
        return s * parts + p

    up = pl.BlockSpec((1, tile, columns), lambda l, s, p, me: (l, jnp.where(s == 0, p, parts - 1), 0))
    down = pl.BlockSpec((1, tile, columns), lambda l, s, p, me: (l, jnp.where(s == 0, 0, p), 0))
    whole = pl.BlockSpec((1, tile, columns), lambda l, s, p, me: (l, me[0] * 2 * parts + row(s, p), 0))
    local = pl.BlockSpec((1, tile, columns), lambda l, s, p, me: (l, row(s, p), 0))
    t_spec = pl.BlockSpec((1, 1, tile, columns), lambda l, s, p, me: (0, l, me[0] * 2 * parts + row(s, p), 0))
    piece = jax.ShapeDtypeStruct((layers, half, columns), jnp.bfloat16)
    moment = jax.ShapeDtypeStruct(m.shape, jnp.float32)
    size = layers * rows * columns
    return pl.pallas_call(
        kernel,
        out_shape=(jax.ShapeDtypeStruct(w.shape, jnp.bfloat16), moment, moment, piece, piece),
        grid_spec=pltpu.PrefetchScalarGridSpec(
            num_scalar_prefetch=1,
            grid=(layers, 2, parts),
            in_specs=[up, down, t_spec, whole, local, local],
            out_specs=(whole, local, local, up, down),
        ),
        cost_estimate=pl.CostEstimate(flops=20 * size, bytes_accessed=26 * size, transcendentals=size),
        name="update",
    )(me, *arrived, term, w, m, v)


def place(axis, hops, whole, pieces, layer, row, half, last):
    layers, rows, columns = pieces[0].shape
    count = whole.shape[1] // (2 * half)

    def kernel(up_ref, down_ref, whole_ref, out_ref, held, in_sems, out_sems):
        del whole_ref
        me = lax.axis_index(axis)
        reads, writes = [], []
        for side, ref in enumerate((up_ref, down_ref)):
            block = lax.rem(me + (count - hops, hops)[side], count)
            start = pl.multiple_of((block * 2 + side) * half, half) + row
            for i in range(layers):
                source = ref.at[i] if last else held.at[side, i]
                if not last:
                    reads.append(pltpu.make_async_copy(ref.at[i], source, in_sems.at[side, i]))
                writes.append(pltpu.make_async_copy(source, out_ref.at[layer + i, pl.ds(start, rows)], out_sems.at[side, i]))
        for read in reads:
            read.start()
        for i, write in enumerate(writes):
            if not last:
                reads[i].wait()
            write.start()
        for write in writes:
            write.wait()

    size = 2 * layers * rows * columns
    return pl.pallas_call(
        kernel,
        out_shape=jax.ShapeDtypeStruct(whole.shape, whole.dtype),
        in_specs=[pl.BlockSpec(memory_space=pltpu.VMEM if last else pl.ANY)] * 2 + [pl.BlockSpec(memory_space=pl.ANY)],
        out_specs=pl.BlockSpec(memory_space=pl.ANY),
        scratch_shapes=[
            pltpu.VMEM((8, 128) if last else (2, layers, rows, columns), whole.dtype),
            pltpu.SemaphoreType.DMA((2, layers)),
            pltpu.SemaphoreType.DMA((2, layers)),
        ],
        input_output_aliases={2: 0},
        compiler_params=pltpu.CompilerParams(vmem_limit_bytes=1 << 20 if last else None),
        cost_estimate=pl.CostEstimate(flops=size, bytes_accessed=4 * size, transcendentals=0),
        name="place",
    )(*pieces, whole)


def first_slice(axis, hops, term, half, row, rows):
    columns = term.shape[3]
    count = term.shape[2] // (2 * half)

    def kernel(term_ref, up_ref, down_ref, sems):
        me = lax.axis_index(axis)
        copies = []
        for side, ref in enumerate((up_ref, down_ref)):
            block = lax.rem(me + (hops, count - hops)[side], count)
            start = pl.multiple_of((block * 2 + side) * half, half) + row
            copies.append(pltpu.make_async_copy(term_ref.at[0, 0, pl.ds(start, rows)], ref.at[0], sems.at[side]))
        for copy in copies:
            copy.start()
        for copy in copies:
            copy.wait()

    piece = jax.ShapeDtypeStruct((1, rows, columns), term.dtype)
    return pl.pallas_call(
        kernel,
        out_shape=(piece, piece),
        in_specs=[pl.BlockSpec(memory_space=pl.ANY)],
        out_specs=(pl.BlockSpec(memory_space=pltpu.VMEM),) * 2,
        scratch_shapes=[pltpu.SemaphoreType.DMA((2,))],
        compiler_params=pltpu.CompilerParams(vmem_limit_bytes=52 << 20),
        cost_estimate=pl.CostEstimate(flops=rows * columns, bytes_accessed=8 * rows * columns, transcendentals=0),
        name="first_slice",
    )(term)


def solution(mesh):
    n = mesh.shape["dp"]
    ways = tuple(tuple((i, (i + to) % n) for i in range(n)) for to in (1, -1))

    def body(*arrays):
        terms, weights, m, v = (arrays[i : i + 3] for i in (0, 3, 6, 9))
        me = lax.axis_index("dp")
        sides = ((0, 1), (1, -1))

        def block(hops, to):
            return lax.rem(me - to * hops + 2 * n, n)

        def own(t, like, hops, part):
            half, (layer, layers, row, rows) = like.shape[1] // 2, part
            starts = [block(-hops, to) * 2 * half + side * half + row for side, to in sides]
            return [lax.dynamic_slice(t, (0, layer, start, 0), (1, layers, rows, t.shape[3]))[0] for start in starts]

        def send(pieces):
            moved = []
            for p, way in zip(pieces, ways, strict=True):
                moved.append(lax.ppermute(p, "dp", way))
            return moved

        def add(a, b):
            return (a.astype(jnp.float32) + b.astype(jnp.float32)).astype(jnp.bfloat16)

        def all_of_it(like):
            return [(0, like.shape[0], 0, like.shape[1] // 2)]

        def small_first(like):
            layers, half = like.shape[0], like.shape[1] // 2
            return [(0, 1, 0, half // 4), (0, 1, half // 4, half - half // 4)] + [(1, layers - 1, 0, half)] * (layers > 1)

        def small_last(like):
            layers, half = like.shape[0], like.shape[1] // 2
            small = half // 64
            ends = [(layers - 1, 1, 0, half - 20 * small), (layers - 1, 1, half - 20 * small, 15 * small), (layers - 1, 1, half - 5 * small, 5 * small)]
            return [(0, layers - 1, 0, half)] * (layers > 1) + ends

        def join(parts):
            first = jnp.concatenate(parts[:2], axis=1)
            return jnp.concatenate([first, *parts[2:]], axis=0) if len(parts) > 2 else first

        order = (0, 1, 2)
        moving = [None] * 3
        new_w, new_m, new_v = [None] * 3, [None] * 3, [None] * 3
        for k in order:
            if k == order[0]:
                half, parts = m[k].shape[1] // 2, small_first(m[k])
                sent = [send(first_slice("dp", n - 1, terms[k], half, row, rows)) for _, _, row, rows in parts[:2]]
                sent += [send(own(terms[k], m[k], n - 1, part)) for part in parts[2:]]
                moving[k] = [join(parts) for parts in zip(*sent, strict=True)]
            else:
                moving[k] = send(own(terms[k], m[k], n - 1, all_of_it(m[k])[0]))
        for hop in range(1, n - 1):
            for k in order:
                moving[k] = send([add(a, b) for a, b in zip(moving[k], own(terms[k], m[k], n - 1 - hop, all_of_it(m[k])[0]), strict=True)])
        at = me[None].astype(jnp.int32)
        for k in order:
            new_w[k], new_m[k], new_v[k], *pieces = update(at, moving[k], terms[k], weights[k], m[k], v[k])
            moving[k] = [(part, send(pieces)) for part in all_of_it(m[k])]
        for hop in range(1, n):
            for k in order:
                here = moving[k]
                if hop < n - 1:
                    parts = small_last(m[k]) if (hop, k) == (n - 2, order[-1]) else all_of_it(m[k])
                    ((_, whole_piece),) = here
                    moving[k] = [
                        (part, send([p[part[0] : part[0] + part[1], part[2] : part[2] + part[3]] for p in whole_piece])) for part in parts
                    ]
                for i, (part, pieces) in enumerate(here):
                    last = (hop, k) == (n - 1, order[-1]) and i >= len(here) - 2
                    new_w[k] = place("dp", hop, new_w[k], pieces, part[0], part[2], m[k].shape[1] // 2, last)
        return (*new_w, *new_m, *new_v)

    all_of, cut = P(None, None, None), P(None, "dp", None)
    return jax.shard_map(
        body,
        mesh=mesh,
        in_specs=(P(("rep", "dp"), None, None, None),) * 3 + (all_of,) * 3 + (cut,) * 6,
        out_specs=(P("rep", None, None),) * 3 + (P("rep", "dp", None),) * 6,
        check_vma=False,
    )
```
